512 devices in a mesh: row: 32 (over z, x), col: 16 (over y, core).
Axes of the slice: x: 4, y: 8, z: 8, core: 2. Of those that a mesh axis runs over, the one named last changes fastest.
Arguments:
- tile_values: bfloat16 [768, 2048, 128], P('row', 'col'), may hold values from -0.02734375 to 0.02734375
- tile_counts: int32 [384, 16], P('row', 'col'), may hold values from 0 to 2, as said below
- tile_cols: int32 [768, 16], P('row', 'col'), may hold values from 0 to 1, as said below
- panels: bfloat16 [49152, 4096], P('row', 'col'), may hold values from -6 to 6
Outputs:
- product: bfloat16 [4096, 4096], P('col', 'row')
The draws below stay inside these ranges and needn't reach their ends.
Inputs may be any that keep to these rules, and one draw needn't show every extreme that they name: `tile_counts`: within each device the filled slots follow block row order; a device holds at most 24 tiles and some device holds exactly 24 in every draw. `tile_cols`: within one block row of a device the filled slots' columns rise strictly; entries of unfilled slots carry no meaning.
All inputs are finite; a program needn't handle non-finite values.
Results may differ from the reference program's by a relative error of at most 0.001.
Values may be sent and summed in bfloat16 or wider, within the bound.
A program may use at most 64 MiB of HBM per device.

```python
import jax
import jax.numpy as jnp
from jax import lax

TILE = 128
NB = 4096
BR_DEV = 12
BC_DEV = 2
CAP = 24
ROWS = 49152
COLS = 4096
N_ROW = 32
N_COL = 16


def tile_pattern(key):
    base = jax.random.fold_in(key, 7)
    key_levels = jax.random.fold_in(base, 1)
    key_rolled = jax.random.fold_in(base, 2)
    key_chosen = jax.random.fold_in(base, 3)
    levels = jax.random.randint(key_levels, (N_ROW, N_COL, BR_DEV, 1), 0, 5)
    chosen = jax.random.randint(key_chosen, (), 0, N_ROW * N_COL)
    device_ids = jnp.arange(N_ROW, dtype=jnp.int32)[:, None] * N_COL + jnp.arange(N_COL, dtype=jnp.int32)[None, :]
    levels = jnp.where((device_ids == chosen)[:, :, None, None], 4, levels)
    rolled = jax.random.randint(key_rolled, (N_ROW, N_COL, BR_DEV, BC_DEV), 0, 4)
    present = (rolled < levels).astype(jnp.int32)
    counts = jnp.sum(present, axis=-1).astype(jnp.int32)
    row_start = (jnp.cumsum(counts, axis=-1) - counts).astype(jnp.int32)
    within = (jnp.cumsum(present, axis=-1) - present).astype(jnp.int32)
    slot_index = jnp.where(present == 1, row_start[..., None] + within, CAP).astype(jnp.int32)
    col_index = jnp.broadcast_to(jnp.arange(BC_DEV, dtype=jnp.int32), present.shape)

    def place_row(slots, values):
        return jnp.zeros((CAP,), jnp.int32).at[slots].set(values, mode='drop')
    columns = jax.vmap(place_row)(slot_index.reshape(N_ROW * N_COL, BR_DEV * BC_DEV), col_index.reshape(N_ROW * N_COL, BR_DEV * BC_DEV))
    return (counts, columns.reshape(N_ROW, N_COL, CAP))


def draw_tile_counts(key, part):
    counts, columns = tile_pattern(key)
    return jnp.transpose(counts, (0, 2, 1)).reshape(N_ROW * BR_DEV, N_COL)


def draw_tile_cols(key, part):
    counts, columns = tile_pattern(key)
    return jnp.transpose(columns, (0, 2, 1)).reshape(N_ROW * CAP, N_COL)


def strengthened(array, stream_key, source, target, blocks, factor):
    owner, partner = [(jnp.arange(array.shape[dim]) // (array.shape[dim] // blocks)).reshape([-1 if axis == dim else 1 for axis in range(array.ndim)]) for dim in (source, target)]
    chosen = jax.random.permutation(stream_key, blocks)[partner]
    strong = (owner == chosen) | (owner == (partner + blocks // 2) % blocks)
    return jnp.where(strong, factor * array, array)


def block_levels(stream_key, dims, split, smallest, top_value):
    factor_of, own = 1.0, jax.random.fold_in(stream_key, 6)
    for axis_at, blocks in split:
        steps = jnp.exp(jax.random.uniform(jax.random.fold_in(own, axis_at), (blocks,), jnp.float32, smallest / len(split), top_value / len(split)))
        factor_of = factor_of * jnp.repeat(steps, dims[axis_at] // blocks).reshape([-1 if axis == axis_at else 1 for axis in range(len(dims))])
    return factor_of


def centred(stream_key, dims, width, reach, cuts=(), kind=jnp.bfloat16):
    entries = width * jax.random.normal(stream_key, dims, jnp.float32)
    if cuts:
        entries = entries * block_levels(stream_key, dims, cuts, -0.22, 0.18)
    return jnp.clip(entries, -reach, reach).astype(kind)


def noise_with(key, shape, width, reach, shards, heavy, held_as=jnp.bfloat16):
    drawn = width * jax.random.normal(key, shape, jnp.float32)
    if shards:
        drawn = drawn * block_levels(key, shape, shards, -0.22, 0.18)
    return jnp.clip(strengthened(drawn, jax.random.fold_in(key, 3), *heavy), -reach, reach).astype(held_as)


def setup_inputs(seed: int = 0) -> dict:
    key_of = jax.random.split(jax.random.key(seed), 5)
    return {
        "tile_values": centred(key_of[0], (N_ROW * CAP, N_COL * TILE, TILE), (TILE * BR_DEV * N_ROW) ** -0.5, 0.02734375, ((0, 32), (1, 16))),
        "tile_counts": draw_tile_counts(jax.random.fold_in(key_of[4], 71), 0),
        "tile_cols": draw_tile_cols(jax.random.fold_in(key_of[4], 71), 0),
        "panels": noise_with(key_of[3], (ROWS, NB), 1.0, 6.0, ((0, 32), (1, 16)), (0, 1, 32, 2.75)),
    }


def reference(tile_values, tile_counts, tile_cols, panels):
    def add_group(row_dev, totals):
        row_dev = jnp.asarray(row_dev).astype(jnp.int32)
        tile_slab = lax.dynamic_slice_in_dim(tile_values, row_dev * CAP, CAP, 0)
        tile_slab = tile_slab.astype(jnp.float32).reshape(CAP, N_COL, TILE, TILE)
        counts = lax.dynamic_slice_in_dim(tile_counts, row_dev * BR_DEV, BR_DEV, 0).astype(jnp.int32)
        columns = lax.dynamic_slice_in_dim(tile_cols, row_dev * CAP, CAP, 0).astype(jnp.int32)
        row_start = (jnp.cumsum(counts, axis=0) - counts).astype(jnp.int32)
        slot_ids = jnp.arange(CAP, dtype=jnp.int32)[:, None, None]
        row_mask = ((slot_ids >= row_start[None]) & (slot_ids < (row_start + counts)[None])).astype(jnp.float32)
        col_mask = (columns[:, None, :] == jnp.arange(BC_DEV, dtype=jnp.int32)[None, :, None]).astype(jnp.float32)
        dense_rows = jnp.einsum("sic,sjc,scab->iacjb", row_mask, col_mask, tile_slab)
        dense_rows = dense_rows.reshape(BR_DEV * TILE, N_COL * BC_DEV * TILE).astype(jnp.bfloat16)
        panel_rows = lax.dynamic_slice_in_dim(panels, row_dev * BR_DEV * TILE, BR_DEV * TILE, 0)
        return totals + lax.dot_general(dense_rows, panel_rows, (((0,), (0,)), ((), ())), preferred_element_type=jnp.float32)

    totals = lax.fori_loop(0, N_ROW, add_group, jnp.zeros((COLS, NB), jnp.float32))
    return totals.astype(jnp.bfloat16)
```

```python
import jax
import jax.numpy as jnp
from jax import lax
from jax.experimental import pallas as pl
from jax.experimental.pallas import tpu as pltpu
from jax.sharding import PartitionSpec as P

MESH = pl.DeviceIdType.MESH
NX, NZ, NY = 4, 8, 8
TILE = 128
STEPS = NY
PIECE = TILE // NZ


def kernel(
    counts, cols, tv_hbm, p_hbm, out_ref,
    tvb, a_own, a_in, bb, give1, keep, x1, give2, x2, zs, zr, cv, obuf,
    load_sem, a_send, a_recv, b_send, b_recv,
    x1_send, x1_recv, x2_send, x2_recv, z_send, z_recv, c_send, c_recv,
):
    row, col = lax.axis_index("row"), lax.axis_index("col")
    z, x = row // NX, lax.rem(row, NX)
    y, k = col // 2, lax.rem(col, 2)

    def dev(z_, x_, y_, k_):
        return (z_ * NX + x_, y_ * 2 + k_)

    right = dev(z, x, lax.rem(y + 1, NY), k)
    left = dev(z, x, lax.rem(y + NY - 1, NY), k)
    sibling = dev(z, x, y, 1 - k)
    flip = x + 1 - 2 * lax.rem(x, 2)
    bit1 = x // 2
    bit0 = lax.rem(bit1 + x, 2)
    swap = k * (NX - 1 - x - flip)
    first_x, second_x = flip + swap, NX - 1 - x - swap
    turn_bit = k * (bit1 - bit0)
    s1, s0 = bit0 + turn_bit, bit1 - turn_bit
    mate1 = dev(z, first_x, y, k)
    mate2 = dev(z, second_x, y, k)

    load_tiles = pltpu.make_async_copy(tv_hbm, tvb, load_sem.at[2])
    load_tiles.start()
    own = []
    for half in range(2):
        copy = pltpu.make_async_copy(
            p_hbm.at[:, pl.ds(half * TILE, TILE)], bb.at[0, 1 - half], load_sem.at[half]
        )
        copy.start()
        own.append(copy)

    barrier = pltpu.get_barrier_semaphore()
    peers = [right, left, sibling, mate1, mate2]
    peers += [dev(lax.rem(z + d, NZ), x, y, k) for d in range(1, NZ)]
    for peer in peers:
        pl.semaphore_signal(barrier, inc=1, device_id=peer, device_id_type=MESH)
    pl.semaphore_wait(barrier, len(peers))

    def ring_copy(src, i, c):
        return pltpu.make_async_remote_copy(
            src_ref=src,
            dst_ref=bb.at[i + 1, c],
            send_sem=b_send.at[i, c],
            recv_sem=b_recv.at[i + 1, c],
            device_id=right if c == 0 else left,
            device_id_type=MESH,
        )

    for i in range(min(2, STEPS - 1)):
        for c in range(2):
            half = (i + c) % 2
            ring_copy(p_hbm.at[:, pl.ds(half * TILE, TILE)], i, c).start()

    load_tiles.wait()

    def build(i, start):
        n = counts[i, 0]
        for b in range(2):
            slot = jnp.minimum(start + jnp.where(n == 2, b, 0), cols.shape[0] - 1)
            valid = jnp.logical_or(n == 2, jnp.logical_and(n == 1, cols[slot, 0] == b))
            tile = tvb[slot].T
            a_own[b * TILE:(b + 1) * TILE, pl.ds(pl.multiple_of(i * TILE, TILE), TILE)] = (
                jnp.where(valid, tile, jnp.zeros_like(tile))
            )
        return start + n

    lax.fori_loop(0, counts.shape[0], build, jnp.int32(0))
    a_copy = pltpu.make_async_remote_copy(
        src_ref=a_own, dst_ref=a_in, send_sem=a_send, recv_sem=a_recv,
        device_id=sibling, device_id_type=MESH,
    )
    a_copy.start()
    own[0].wait()
    own[1].wait()
    a_copy.wait()

    def x1_copy(t):
        return pltpu.make_async_remote_copy(
            src_ref=give1.at[t], dst_ref=x1.at[t],
            send_sem=x1_send.at[t], recv_sem=x1_recv.at[t], device_id=mate1, device_id_type=MESH,
        )

    def x2_copy(t):
        return pltpu.make_async_remote_copy(
            src_ref=give2.at[t], dst_ref=x2.at[t],
            send_sem=x2_send.at[t], recv_sem=x2_recv.at[t], device_id=mate2, device_id_type=MESH,
        )

    def owner_row(c, t):
        far = (t + 1) // 2
        j = lax.rem(y + NY + (far if c else -far), NY)
        half = lax.rem(t + 1 + c, 2)
        return j, 2 * k + half

    def take_block(t):
        for c in range(2):
            ring_copy(bb.at[t, c], t - 1, c).wait_recv()

            @pl.when(t < STEPS - 2)
            def _():
                ring_copy(bb.at[t, c], t + 1, c).start()

    def step(it, carry):
        @pl.when(jnp.logical_and(it >= 1, it < STEPS))
        def _():
            take_block(it)

        @pl.when(it < STEPS)
        def _():
            t = it
            for turn in range(2):
                half = (1 - s1) if turn == 0 else s1
                both = jnp.concatenate([bb[t, 0], bb[t, 1]], axis=1)
                lhs = jnp.where(half == k, a_own[...], a_in[...])
                value = jnp.dot(lhs, both, preferred_element_type=jnp.float32)
                target = give1 if turn == 0 else keep
                target[t] = value.reshape(2, NZ, PIECE, 256)
                if turn == 0:
                    x1_copy(t).start()

        @pl.when(jnp.logical_and(it >= 1, it < STEPS + 1))
        def _():
            t = it - 1
            x1_copy(t).wait_recv()
            low, high = keep[t, 0] + x1[t, 0], keep[t, 1] + x1[t, 1]
            give2[t] = jnp.where(s0 == 0, high, low)
            x2_copy(t).start()
            zs[t] = jnp.where(s0 == 0, low, high)

        @pl.when(jnp.logical_and(it >= 2, it < STEPS + 2))
        def _():
            t = it - 2
            x2_copy(t).wait_recv()
            zs[t] = zs[t] + x2[t]
            for d in sorted(range(1, NZ), key=lambda d: abs(d - NZ // 2)):
                peer = lax.rem(z + d, NZ)
                pltpu.make_async_remote_copy(
                    src_ref=zs.at[t, peer],
                    dst_ref=zr.at[t, d - 1],
                    send_sem=z_send.at[t], recv_sem=z_recv.at[t],
                    device_id=dev(peer, x, y, k), device_id_type=MESH,
                ).start()

        @pl.when(it >= 3)
        def _():
            t = it - 3
            pltpu.make_async_copy(zr.at[t], zr.at[t], z_recv.at[t]).wait()
            total = zs[t, z]
            for d in range(NZ - 1):
                total = total + zr[t, d]
            for c in range(2):
                cv[t, c] = total[:, c * TILE:(c + 1) * TILE].astype(jnp.bfloat16)
            dst_core = s1
            for c in range(2):
                j, owner_x = owner_row(c, t)
                me = jnp.logical_and(
                    jnp.logical_and(j == z, owner_x == x), dst_core == k
                )
                dst = obuf.at[s0 * NZ + z]

                @pl.when(me)
                def _():
                    copy = pltpu.make_async_copy(cv.at[t, c], dst, load_sem.at[0])
                    copy.start()
                    copy.wait()

                @pl.when(jnp.logical_not(me))
                def _():
                    pltpu.make_async_remote_copy(
                        src_ref=cv.at[t, c], dst_ref=dst,
                        send_sem=c_send.at[t, c], recv_sem=c_recv,
                        device_id=dev(j, owner_x, y, dst_core), device_id_type=MESH,
                    ).start()
        return carry

    lax.fori_loop(0, STEPS + 3, step, 0)

    has_own = jnp.logical_and(x // 2 == k, s1 == k)

    @pl.when(has_own)
    def _():
        others = obuf.at[pl.ds(0, 2 * NZ - 1)]
        pltpu.make_async_copy(others, others, c_recv).wait()

    @pl.when(jnp.logical_not(has_own))
    def _():
        pltpu.make_async_copy(obuf, obuf, c_recv).wait()

    out_ref[...] = obuf[...].reshape(256, TILE)

    def drain(t, carry):
        x1_copy(t).wait_send()
        x2_copy(t).wait_send()
        pltpu.make_async_copy(zr.at[t], zr.at[t], z_send.at[t]).wait()
        for c in range(2):
            @pl.when(t < STEPS - 1)
            def _():
                ring_copy(bb.at[t, c], t, c).wait_send()
            j, owner_x = owner_row(c, t)
            me = jnp.logical_and(
                jnp.logical_and(j == z, owner_x == x), s1 == k
            )

            @pl.when(jnp.logical_not(me))
            def _():
                pltpu.make_async_copy(cv.at[t, c], cv.at[t, c], c_send.at[t, c]).wait()
        return carry

    lax.fori_loop(0, STEPS, drain, 0)


def per_device(tile_values, tile_counts, tile_cols, panels):
    bf16, f32 = jnp.bfloat16, jnp.float32
    dma = pltpu.SemaphoreType.DMA
    return pl.pallas_call(
        kernel,
        out_shape=jax.ShapeDtypeStruct((256, TILE), bf16),
        in_specs=[
            pl.BlockSpec(memory_space=pltpu.SMEM),
            pl.BlockSpec(memory_space=pltpu.SMEM),
            pl.BlockSpec(memory_space=pl.ANY),
            pl.BlockSpec(memory_space=pl.ANY),
        ],
        out_specs=pl.BlockSpec(memory_space=pltpu.VMEM),
        scratch_shapes=[
            pltpu.VMEM(tile_values.shape, bf16),
            pltpu.VMEM((256, panels.shape[0]), bf16),
            pltpu.VMEM((256, panels.shape[0]), bf16),
            pltpu.VMEM((STEPS, 2, panels.shape[0], TILE), bf16),
            pltpu.VMEM((STEPS, 2, NZ, PIECE, 256), f32),
            pltpu.VMEM((STEPS, 2, NZ, PIECE, 256), f32),
            pltpu.VMEM((STEPS, 2, NZ, PIECE, 256), f32),
            pltpu.VMEM((STEPS, NZ, PIECE, 256), f32),
            pltpu.VMEM((STEPS, NZ, PIECE, 256), f32),
            pltpu.VMEM((STEPS, NZ, PIECE, 256), f32),
            pltpu.VMEM((STEPS, NZ - 1, PIECE, 256), f32),
            pltpu.VMEM((STEPS, 2, PIECE, TILE), bf16),
            pltpu.VMEM((2 * NZ, PIECE, TILE), bf16),
            dma((3,)), dma, dma,
            dma((STEPS - 1, 2)), dma((STEPS, 2)),
            dma((STEPS,)), dma((STEPS,)), dma((STEPS,)), dma((STEPS,)),
            dma((STEPS,)), dma((STEPS,)), dma((STEPS, 2)), dma,
        ],
        compiler_params=pltpu.CompilerParams(
            collective_id=0, has_side_effects=True, vmem_limit_bytes=48 * 1024 * 1024
        ),
    )(tile_counts, tile_cols, tile_values, panels)


def solution(mesh):
    return jax.shard_map(
        per_device,
        mesh=mesh,
        in_specs=(P("row", "col", None), P("row", "col"), P("row", "col"), P("row", "col")),
        out_specs=P("col", "row"),
        check_vma=False,
    )
```

```python
import jax
import jax.numpy as jnp
from jax import lax
from jax.experimental import pallas as pl
from jax.experimental.pallas import tpu as pltpu
from jax.sharding import PartitionSpec as P

MESH = pl.DeviceIdType.MESH
NX, NZ, NY = 4, 8, 8
TILE = 128
STEPS = NY
PIECE = TILE // NZ


def kernel(
    counts, cols, tv_hbm, p_hbm, out_ref,
    tvb, a_own, a_in, bb, give1, keep, x1, give2, x2, zs, zr, cv, obuf,
    load_sem, a_send, a_recv, b_send, b_recv,
    x1_send, x1_recv, x2_send, x2_recv, z_send, z_recv, c_send, c_recv, known,
):
    row, col = lax.axis_index("row"), lax.axis_index("col")
    z, x = row // NX, lax.rem(row, NX)
    y, k = col // 2, lax.rem(col, 2)

    def dev(z_, x_, y_, k_):
        return (z_ * NX + x_, y_ * 2 + k_)

    right = dev(z, x, lax.rem(y + 1, NY), k)
    left = dev(z, x, lax.rem(y + NY - 1, NY), k)
    sibling = dev(z, x, y, 1 - k)
    flip = x + 1 - 2 * lax.rem(x, 2)
    bit1 = x // 2
    bit0 = lax.rem(bit1 + x, 2)
    swap = k * (NX - 1 - x - flip)
    first_x, second_x = flip + swap, NX - 1 - x - swap
    turn_bit = k * (bit1 - bit0)
    s1, s0 = bit0 + turn_bit, bit1 - turn_bit
    mate1 = dev(z, first_x, y, k)
    mate2 = dev(z, second_x, y, k)

    load_tiles = pltpu.make_async_copy(tv_hbm, tvb, load_sem.at[2])
    load_tiles.start()
    own = []
    for half in range(2):
        copy = pltpu.make_async_copy(
            p_hbm.at[:, pl.ds(half * TILE, TILE)], bb.at[0, 1 - half], load_sem.at[half]
        )
        copy.start()
        own.append(copy)

    barrier = pltpu.get_barrier_semaphore()
    above = dev(lax.rem(z + 1, NZ), x, y, k)
    below = dev(lax.rem(z + NZ - 1, NZ), x, y, k)
    peers = [right, left, sibling, mate1, mate2, above, below]
    for peer in peers:
        pl.semaphore_signal(barrier, inc=1, device_id=peer, device_id_type=MESH)
    pl.semaphore_wait(barrier, len(peers))

    def tell(r):
        for side, peer in ((0, above), (1, below)):
            pl.semaphore_signal(known.at[r, side], inc=1, device_id=peer, device_id_type=MESH)

    def hear(r):
        for side in range(2):
            pl.semaphore_wait(known.at[r, side], 1)

    def ring_copy(src, i, c):
        return pltpu.make_async_remote_copy(
            src_ref=src,
            dst_ref=bb.at[i + 1, c],
            send_sem=b_send.at[i, c],
            recv_sem=b_recv.at[i + 1, c],
            device_id=right if c == 0 else left,
            device_id_type=MESH,
        )

    for i in range(min(2, STEPS - 1)):
        for c in range(2):
            half = (i + c) % 2
            ring_copy(p_hbm.at[:, pl.ds(half * TILE, TILE)], i, c).start()
    tell(0)

    load_tiles.wait()

    def build(i, start):
        n = counts[0, i]
        for b in range(2):
            slot = jnp.minimum(start + jnp.where(n == 2, b, 0), cols.shape[1] - 1)
            valid = jnp.logical_or(n == 2, jnp.logical_and(n == 1, cols[0, slot] == b))
            tile = tvb[slot].T
            a_own[b * TILE:(b + 1) * TILE, pl.ds(pl.multiple_of(i * TILE, TILE), TILE)] = (
                jnp.where(valid, tile, jnp.zeros_like(tile))
            )
        return start + n

    lax.fori_loop(0, counts.shape[1], build, jnp.int32(0))
    a_copy = pltpu.make_async_remote_copy(
        src_ref=a_own, dst_ref=a_in, send_sem=a_send, recv_sem=a_recv,
        device_id=sibling, device_id_type=MESH,
    )
    a_copy.start()
    hear(0)
    tell(1)
    own[0].wait()
    own[1].wait()
    a_copy.wait()
    hear(1)
    tell(2)

    def x1_copy(t, piece):
        return pltpu.make_async_remote_copy(
            src_ref=give1.at[t, piece], dst_ref=x1.at[t, piece],
            send_sem=x1_send.at[t, piece], recv_sem=x1_recv.at[t, piece],
            device_id=mate1, device_id_type=MESH,
        )

    def x2_copy(t):
        return pltpu.make_async_remote_copy(
            src_ref=give2.at[t], dst_ref=x2.at[t],
            send_sem=x2_send.at[t], recv_sem=x2_recv.at[t], device_id=mate2, device_id_type=MESH,
        )

    def owner_row(c, t):
        far = (t + 1) // 2
        j = lax.rem(y + NY + (far if c else -far), NY)
        half = lax.rem(t + 1 + c, 2)
        return j, 2 * k + half

    def take_block(t):
        for c in range(2):
            ring_copy(bb.at[t, c], t - 1, c).wait_recv()

            @pl.when(t < STEPS - 2)
            def _():
                ring_copy(bb.at[t, c], t + 1, c).start()

    def step(it, carry):
        @pl.when(jnp.logical_and(it >= 1, it < STEPS))
        def _():
            take_block(it)

        @pl.when(it < STEPS)
        def _():
            t = it
            both = jnp.concatenate([bb[t, 0], bb[t, 1]], axis=1)
            for half, target in ((1 - s1, give1), (s1, keep)):
                for piece in range(2):
                    sub = (1 - s0) if piece == 0 else s0
                    rows = pl.ds(pl.multiple_of(sub * TILE, TILE), TILE)
                    lhs = jnp.where(half == k, a_own[rows], a_in[rows])
                    value = jnp.dot(lhs, both, preferred_element_type=jnp.float32)
                    target[t, piece] = value.reshape(NZ, PIECE, 256)
                    if target is give1:
                        x1_copy(t, piece).start()

        @pl.when(it == 0)
        def _():
            hear(2)

        @pl.when(jnp.logical_and(it >= 1, it < STEPS + 1))
        def _():
            t = it - 1
            x1_copy(t, 1).wait_recv()
            x2_copy(t).wait_recv()
            zs[t] = keep[t, 1] + x1[t, 1] + x2[t]
            for d in sorted(range(1, NZ), key=lambda d: abs(d - NZ // 2)):
                peer = lax.rem(z + d, NZ)
                pltpu.make_async_remote_copy(
                    src_ref=zs.at[t, peer],
                    dst_ref=zr.at[t, d - 1],
                    send_sem=z_send.at[t], recv_sem=z_recv.at[t],
                    device_id=dev(peer, x, y, k), device_id_type=MESH,
                ).start()

        @pl.when(it >= 2)
        def _():
            t = it - 2
            pltpu.make_async_copy(zr.at[t], zr.at[t], z_recv.at[t]).wait()
            total = zs[t, z]
            for d in range(NZ - 1):
                total = total + zr[t, d]
            for c in range(2):
                cv[t, c] = total[:, c * TILE:(c + 1) * TILE].astype(jnp.bfloat16)
            dst_core = s1
            for c in range(2):
                j, owner_x = owner_row(c, t)
                me = jnp.logical_and(
                    jnp.logical_and(j == z, owner_x == x), dst_core == k
                )
                dst = obuf.at[s0 * NZ + z]

                @pl.when(me)
                def _():
                    copy = pltpu.make_async_copy(cv.at[t, c], dst, load_sem.at[0])
                    copy.start()
                    copy.wait()

                @pl.when(jnp.logical_not(me))
                def _():
                    pltpu.make_async_remote_copy(
                        src_ref=cv.at[t, c], dst_ref=dst,
                        send_sem=c_send.at[t, c], recv_sem=c_recv,
                        device_id=dev(j, owner_x, y, dst_core), device_id_type=MESH,
                    ).start()
        @pl.when(it < STEPS)
        def _():
            t = it
            x1_copy(t, 0).wait_recv()
            give2[t] = keep[t, 0] + x1[t, 0]
            x2_copy(t).start()

        return carry

    lax.fori_loop(0, STEPS + 2, step, 0)

    has_own = jnp.logical_and(x // 2 == k, s1 == k)

    @pl.when(has_own)
    def _():
        others = obuf.at[pl.ds(0, 2 * NZ - 1)]
        pltpu.make_async_copy(others, others, c_recv).wait()

    @pl.when(jnp.logical_not(has_own))
    def _():
        pltpu.make_async_copy(obuf, obuf, c_recv).wait()

    out_ref[...] = obuf[...].reshape(256, TILE)

    def drain(t, carry):
        x1_copy(t, 0).wait_send()
        x1_copy(t, 1).wait_send()
        x2_copy(t).wait_send()
        pltpu.make_async_copy(zr.at[t], zr.at[t], z_send.at[t]).wait()
        for c in range(2):
            @pl.when(t < STEPS - 1)
            def _():
                ring_copy(bb.at[t, c], t, c).wait_send()
            j, owner_x = owner_row(c, t)
            me = jnp.logical_and(
                jnp.logical_and(j == z, owner_x == x), s1 == k
            )

            @pl.when(jnp.logical_not(me))
            def _():
                pltpu.make_async_copy(cv.at[t, c], cv.at[t, c], c_send.at[t, c]).wait()
        return carry

    lax.fori_loop(0, STEPS, drain, 0)


def per_device(tile_values, tile_counts, tile_cols, panels):
    bf16, f32 = jnp.bfloat16, jnp.float32
    dma = pltpu.SemaphoreType.DMA
    return pl.pallas_call(
        kernel,
        out_shape=jax.ShapeDtypeStruct((256, TILE), bf16),
        in_specs=[
            pl.BlockSpec(memory_space=pltpu.SMEM),
            pl.BlockSpec(memory_space=pltpu.SMEM),
            pl.BlockSpec(memory_space=pl.ANY),
            pl.BlockSpec(memory_space=pl.ANY),
        ],
        out_specs=pl.BlockSpec(memory_space=pltpu.VMEM),
        scratch_shapes=[
            pltpu.VMEM(tile_values.shape, bf16),
            pltpu.VMEM((256, panels.shape[0]), bf16),
            pltpu.VMEM((256, panels.shape[0]), bf16),
            pltpu.VMEM((STEPS, 2, panels.shape[0], TILE), bf16),
            pltpu.VMEM((STEPS, 2, NZ, PIECE, 256), f32),
            pltpu.VMEM((STEPS, 2, NZ, PIECE, 256), f32),
            pltpu.VMEM((STEPS, 2, NZ, PIECE, 256), f32),
            pltpu.VMEM((STEPS, NZ, PIECE, 256), f32),
            pltpu.VMEM((STEPS, NZ, PIECE, 256), f32),
            pltpu.VMEM((STEPS, NZ, PIECE, 256), f32),
            pltpu.VMEM((STEPS, NZ - 1, PIECE, 256), f32),
            pltpu.VMEM((STEPS, 2, PIECE, TILE), bf16),
            pltpu.VMEM((2 * NZ, PIECE, TILE), bf16),
            dma((3,)), dma, dma,
            dma((STEPS - 1, 2)), dma((STEPS, 2)),
            dma((STEPS, 2)), dma((STEPS, 2)), dma((STEPS,)), dma((STEPS,)),
            dma((STEPS,)), dma((STEPS,)), dma((STEPS, 2)), dma,
            pltpu.SemaphoreType.REGULAR((3, 2)),
        ],
        compiler_params=pltpu.CompilerParams(
            collective_id=0, has_side_effects=True, vmem_limit_bytes=60 * 1024 * 1024
        ),
    )(tile_counts.T, tile_cols.T, tile_values, panels)


def solution(mesh):
    return jax.shard_map(
        per_device,
        mesh=mesh,
        in_specs=(P("row", "col", None), P("row", "col"), P("row", "col"), P("row", "col")),
        out_specs=P("col", "row"),
        check_vma=False,
    )
```

```python
import jax
import jax.numpy as jnp
from jax import lax
from jax.experimental import pallas as pl
from jax.experimental.pallas import tpu as pltpu
from jax.sharding import PartitionSpec as P

MESH = pl.DeviceIdType.MESH
NX, NZ, NY = 4, 8, 8
TILE = 128
STEPS = NY
LAST = STEPS - 1
PIECE = 2 * TILE // NZ


def kernel(
    counts, cols, tv_hbm, p_hbm, out_ref,
    tvb, a_own, a_in, a_mate, bb, give, keep, x2, zs, zr, cv, obuf,
    load_sem, a_send, a_recv, b_send, b_recv, e_send, e_recv, m_send, m_recv,
    x2_send, x2_recv, z_send, z_recv, c_send, c_recv, known,
):
    row, col = lax.axis_index("row"), lax.axis_index("col")
    z, x = row // NX, lax.rem(row, NX)
    y, k = col // 2, lax.rem(col, 2)
    depth = p_hbm.shape[0]
    half_depth = depth // 2

    def dev(z_, x_, y_, k_):
        return (z_ * NX + x_, y_ * 2 + k_)

    right = dev(z, x, lax.rem(y + 1, NY), k)
    left = dev(z, x, lax.rem(y + NY - 1, NY), k)
    above = dev(lax.rem(z + 1, NZ), x, y, k)
    below = dev(lax.rem(z + NZ - 1, NZ), x, y, k)
    sibling = dev(z, x, y, 1 - k)
    flip = x + 1 - 2 * lax.rem(x, 2)
    bit1 = x // 2
    bit0 = lax.rem(bit1 + x, 2)
    swap = k * (NX - 1 - x - flip)
    turn_bit = k * (bit1 - bit0)
    s1, s0 = bit0 + turn_bit, bit1 - turn_bit
    mate1 = dev(z, flip + swap, y, k)
    mate2 = dev(z, NX - 1 - x - swap, y, k)
    owner_x = 2 * k + s1

    def remote(src, dst, send, recv, to):
        return pltpu.make_async_remote_copy(
            src_ref=src, dst_ref=dst, send_sem=send, recv_sem=recv,
            device_id=to, device_id_type=MESH,
        )

    load_tiles = pltpu.make_async_copy(tv_hbm, tvb, load_sem.at[0])
    load_tiles.start()
    own_columns = p_hbm.at[:, pl.ds(pl.multiple_of(s1 * TILE, TILE), TILE)]
    mate_columns = p_hbm.at[:, pl.ds(pl.multiple_of((1 - s1) * TILE, TILE), TILE)]
    load_own = pltpu.make_async_copy(own_columns, bb.at[0, 0], load_sem.at[1])
    load_own.start()

    barrier = pltpu.get_barrier_semaphore()
    peers = [right, left, sibling, mate1, mate2, above, below]
    for peer in peers:
        pl.semaphore_signal(barrier, inc=1, device_id=peer, device_id_type=MESH)
    pl.semaphore_wait(barrier, len(peers))

    def tell(r):
        for side, peer in ((0, above), (1, below)):
            pl.semaphore_signal(known.at[r, side], inc=1, device_id=peer, device_id_type=MESH)

    def hear(r):
        for side in range(2):
            pl.semaphore_wait(known.at[r, side], 1)

    def ring_copy(src, i, c):
        return remote(src, bb.at[i + 1, c], b_send.at[i, c], b_recv.at[i + 1, c], left if c else right)

    def end_copy(part, c):
        rows = pl.ds(c * half_depth, half_depth)
        src = bb.at[LAST - 2 + part, c, rows]
        return remote(src, bb.at[LAST, part, rows], e_send.at[part, c], e_recv.at[part, c], left if c else right)

    first = [ring_copy(own_columns, 0, c) for c in range(2)]
    for copy in first:
        copy.start()
    merge = remote(mate_columns, bb.at[0, 1], m_send.at[2], m_recv.at[2], mate1)
    merge.start()
    tell(0)

    load_tiles.wait()

    def build(i, start):
        n = counts[0, i]
        for b in range(2):
            slot = jnp.minimum(start + jnp.where(n == 2, b, 0), cols.shape[1] - 1)
            valid = jnp.logical_or(n == 2, jnp.logical_and(n == 1, cols[0, slot] == b))
            tile = tvb[slot].T
            a_own[b * TILE:(b + 1) * TILE, pl.ds(pl.multiple_of(i * TILE, TILE), TILE)] = (
                jnp.where(valid, tile, jnp.zeros_like(tile))
            )
        return start + n

    lax.fori_loop(0, counts.shape[1], build, jnp.int32(0))
    a_copy = remote(a_own, a_in, a_send, a_recv, sibling)
    a_copy.start()
    mate_own = remote(a_own, a_mate.at[0], m_send.at[0], m_recv.at[0], mate1)
    mate_own.start()
    hear(0)
    tell(1)
    a_copy.wait()
    mate_in = remote(a_in, a_mate.at[1], m_send.at[1], m_recv.at[1], mate1)
    mate_in.start()
    hear(1)
    tell(2)

    merge.wait_recv()
    second = [ring_copy(bb.at[0, 1], 1, c) for c in range(2)]
    for copy in second:
        copy.start()

    sent = first + second + [mate_own, mate_in, merge]

    def take(t):
        for c in range(2):
            if t == LAST:
                for part in range(2):
                    end_copy(part, c).wait_recv()
                continue
            ring_copy(bb.at[0, 0], t - 1, c).wait_recv()
            if t <= LAST - 3:
                copy = ring_copy(bb.at[t, c], t + 1, c)
            else:
                copy = end_copy(t - (LAST - 2), c)
            copy.start()
            sent.append(copy)

    def blocks(s):
        if s == 0:
            return bb[0, 0], bb[0, 1]
        if s == LAST:
            return bb[LAST, 0], bb[LAST, 1]
        if s % 2:
            return bb[s, 0], bb[s + 1, 0]
        return bb[s - 1, 1], bb[s, 1]

    def x2_copy(s):
        return remote(give.at[s], x2.at[s], x2_send.at[s], x2_recv.at[s], mate2)

    def multiply(s):
        mine, mates = blocks(s)
        for core, target in ((1 - s0, give), (s0, keep)):
            lhs = jnp.where(core == k, a_own[...], a_in[...])
            value = jnp.dot(lhs, mine, preferred_element_type=jnp.float32)
            lhs = jnp.where(core == k, a_mate[0], a_mate[1])
            value += jnp.dot(lhs, mates, preferred_element_type=jnp.float32)
            target[s] = value.reshape(NZ, PIECE, TILE)
            if target is give:
                copy = x2_copy(s)
                copy.start()
                sent.append(copy)

    def spread(s):
        x2_copy(s).wait_recv()
        zs[s] = keep[s] + x2[s]
        for d in sorted(range(1, NZ), key=lambda d: abs(d - NZ // 2)):
            peer = lax.rem(z + d, NZ)
            remote(
                zs.at[s, peer], zr.at[s, d - 1], z_send.at[s], z_recv.at[s], dev(peer, x, y, k)
            ).start()

    def owner(s):
        j = lax.rem(y + NY + (-((s + 1) // 2) if s % 2 else s // 2), NY)
        me = jnp.logical_and(j == z, jnp.logical_and(owner_x == x, s0 == k))
        return j, me

    def deliver(s):
        pltpu.make_async_copy(zr.at[s], zr.at[s], z_recv.at[s]).wait()
        total = zs[s, z]
        for d in range(NZ - 1):
            total = total + zr[s, d]
        cv[s] = total.astype(jnp.bfloat16)
        j, me = owner(s)

        @pl.when(me)
        def _():
            copy = pltpu.make_async_copy(cv.at[s], obuf.at[z], load_sem.at[0])
            copy.start()
            copy.wait()

        @pl.when(jnp.logical_not(me))
        def _():
            remote(cv.at[s], obuf.at[z], c_send.at[s], c_recv, dev(j, owner_x, y, s0)).start()

    load_own.wait()
    take(1)
    if LAST > 2:
        take(2)
    hear(2)
    mate_own.wait_recv()
    mate_in.wait_recv()
    for s in range(STEPS + 2):
        if s == LAST:
            take(LAST)
        elif 2 <= s < LAST - 1:
            take(s + 1)
        if s < STEPS:
            multiply(s)
        if 1 <= s < STEPS + 1:
            spread(s - 1)
        if s >= 2:
            deliver(s - 2)

    has_own = jnp.logical_and(owner_x == x, s0 == k)

    @pl.when(has_own)
    def _():
        others = obuf.at[pl.ds(0, NZ - 1)]
        pltpu.make_async_copy(others, others, c_recv).wait()

    @pl.when(jnp.logical_not(has_own))
    def _():
        pltpu.make_async_copy(obuf, obuf, c_recv).wait()

    out_ref[...] = obuf[...].reshape(2 * TILE, TILE)

    for copy in sent:
        copy.wait_send()
    for s in range(STEPS):
        pltpu.make_async_copy(zr.at[s], zr.at[s], z_send.at[s]).wait()
        _, me = owner(s)

        @pl.when(jnp.logical_not(me))
        def _():
            pltpu.make_async_copy(cv.at[s], cv.at[s], c_send.at[s]).wait()


def per_device(tile_values, tile_counts, tile_cols, panels):
    bf16, f32 = jnp.bfloat16, jnp.float32
    dma = pltpu.SemaphoreType.DMA
    depth = panels.shape[0]
    return pl.pallas_call(
        kernel,
        out_shape=jax.ShapeDtypeStruct((2 * TILE, TILE), bf16),
        in_specs=[
            pl.BlockSpec(memory_space=pltpu.SMEM),
            pl.BlockSpec(memory_space=pltpu.SMEM),
            pl.BlockSpec(memory_space=pl.ANY),
            pl.BlockSpec(memory_space=pl.ANY),
        ],
        out_specs=pl.BlockSpec(memory_space=pltpu.VMEM),
        scratch_shapes=[
            pltpu.VMEM(tile_values.shape, bf16),
            pltpu.VMEM((2 * TILE, depth), bf16),
            pltpu.VMEM((2 * TILE, depth), bf16),
            pltpu.VMEM((2, 2 * TILE, depth), bf16),
            pltpu.VMEM((STEPS, 2, depth, TILE), bf16),
            pltpu.VMEM((STEPS, NZ, PIECE, TILE), f32),
            pltpu.VMEM((STEPS, NZ, PIECE, TILE), f32),
            pltpu.VMEM((STEPS, NZ, PIECE, TILE), f32),
            pltpu.VMEM((STEPS, NZ, PIECE, TILE), f32),
            pltpu.VMEM((STEPS, NZ - 1, PIECE, TILE), f32),
            pltpu.VMEM((STEPS, PIECE, TILE), bf16),
            pltpu.VMEM((NZ, PIECE, TILE), bf16),
            dma((2,)), dma, dma,
            dma((STEPS, 2)), dma((STEPS, 2)), dma((2, 2)), dma((2, 2)), dma((3,)), dma((3,)),
            dma((STEPS,)), dma((STEPS,)), dma((STEPS,)), dma((STEPS,)), dma((STEPS,)), dma,
            pltpu.SemaphoreType.REGULAR((3, 2)),
        ],
        compiler_params=pltpu.CompilerParams(
            collective_id=0, has_side_effects=True, vmem_limit_bytes=60 * 1024 * 1024
        ),
    )(tile_counts.T, tile_cols.T, tile_values, panels)


def solution(mesh):
    return jax.shard_map(
        per_device,
        mesh=mesh,
        in_specs=(P("row", "col", None), P("row", "col"), P("row", "col"), P("row", "col")),
        out_specs=P("col", "row"),
        check_vma=False,
    )
```

```python
import jax
import jax.numpy as jnp
from jax import lax
from jax.experimental import pallas as pl
from jax.experimental.pallas import tpu as pltpu
from jax.sharding import PartitionSpec as P

MESH = pl.DeviceIdType.MESH
NX, NZ, NY = 4, 8, 8
TILE = 128
STEPS = NY
LAST = STEPS - 1
PIECE = 2 * TILE // NZ


def kernel(
    counts, cols, tv_hbm, p_hbm, out_ref,
    tvb, a_own, a_in, a_mate, bb, give, keep, x2, zs, zr, cv, obuf,
    load_sem, a_send, a_recv, b_send, b_recv, e_send, e_recv, m_send, m_recv,
    x2_send, x2_recv, z_send, z_recv, c_send, c_recv, known,
):
    row, col = lax.axis_index("row"), lax.axis_index("col")
    z, x = row // NX, lax.rem(row, NX)
    y, k = col // 2, lax.rem(col, 2)
    depth = p_hbm.shape[0]
    half_depth = depth // 2

    def dev(z_, x_, y_, k_):
        return (z_ * NX + x_, y_ * 2 + k_)

    right = dev(z, x, lax.rem(y + 1, NY), k)
    left = dev(z, x, lax.rem(y + NY - 1, NY), k)
    above = dev(lax.rem(z + 1, NZ), x, y, k)
    below = dev(lax.rem(z + NZ - 1, NZ), x, y, k)
    sibling = dev(z, x, y, 1 - k)
    flip = x + 1 - 2 * lax.rem(x, 2)
    bit1 = x // 2
    bit0 = lax.rem(bit1 + x, 2)
    swap = k * (NX - 1 - x - flip)
    turn_bit = k * (bit1 - bit0)
    s1, s0 = bit0 + turn_bit, bit1 - turn_bit
    mate1 = dev(z, flip + swap, y, k)
    mate2 = dev(z, NX - 1 - x - swap, y, k)
    owner_x = 2 * k + s1

    def remote(src, dst, send, recv, to):
        return pltpu.make_async_remote_copy(
            src_ref=src, dst_ref=dst, send_sem=send, recv_sem=recv,
            device_id=to, device_id_type=MESH,
        )

    load_tiles = pltpu.make_async_copy(tv_hbm, tvb, load_sem.at[0])
    load_tiles.start()
    own_columns = p_hbm.at[:, pl.ds(pl.multiple_of(s1 * TILE, TILE), TILE)]
    mate_columns = p_hbm.at[:, pl.ds(pl.multiple_of((1 - s1) * TILE, TILE), TILE)]
    load_own = pltpu.make_async_copy(own_columns, bb.at[0, 0], load_sem.at[1])
    load_own.start()

    barrier = pltpu.get_barrier_semaphore()
    peers = [right, left, sibling, mate1, mate2, above, below]
    for peer in peers:
        pl.semaphore_signal(barrier, inc=1, device_id=peer, device_id_type=MESH)
    pl.semaphore_wait(barrier, len(peers))

    def tell(r):
        for side, peer in ((0, above), (1, below)):
            pl.semaphore_signal(known.at[r, side], inc=1, device_id=peer, device_id_type=MESH)

    def hear(r):
        for side in range(2):
            pl.semaphore_wait(known.at[r, side], 1)

    def ring_copy(src, i, c):
        return remote(src, bb.at[i + 1, c], b_send.at[i, c], b_recv.at[i + 1, c], left if c else right)

    def end_copy(part, c):
        rows = pl.ds(c * half_depth, half_depth)
        src = bb.at[LAST - 2 + part, c, rows]
        return remote(src, bb.at[LAST, part, rows], e_send.at[part, c], e_recv.at[part, c], left if c else right)

    first = [ring_copy(own_columns, 0, c) for c in range(2)]
    for copy in first:
        copy.start()
    merge = remote(mate_columns, bb.at[0, 1], m_send.at[2], m_recv.at[2], mate1)
    merge.start()
    tell(0)

    load_tiles.wait()

    def build(i, start):
        n = counts[0, i]
        for b in range(2):
            slot = jnp.minimum(start + jnp.where(n == 2, b, 0), cols.shape[1] - 1)
            valid = jnp.logical_or(n == 2, jnp.logical_and(n == 1, cols[0, slot] == b))
            tile = tvb[slot].T
            tile = jnp.where(valid, tile, jnp.zeros_like(tile))
            for q in range(TILE // PIECE):
                place = lax.rem(b * (TILE // PIECE) + q - z + 2 * NZ - 2, NZ)
                rows = pl.ds(pl.multiple_of(place * PIECE, PIECE), PIECE)
                lanes = pl.ds(pl.multiple_of(i * TILE, TILE), TILE)
                a_own[rows, lanes] = tile[q * PIECE:(q + 1) * PIECE]
        return start + n

    lax.fori_loop(0, counts.shape[1], build, jnp.int32(0))
    a_copy = remote(a_own, a_in, a_send, a_recv, sibling)
    a_copy.start()
    mate_own = remote(a_own, a_mate.at[0], m_send.at[0], m_recv.at[0], mate1)
    mate_own.start()
    hear(0)
    tell(1)
    a_copy.wait()
    mate_in = remote(a_in, a_mate.at[1], m_send.at[1], m_recv.at[1], mate1)
    mate_in.start()
    hear(1)
    tell(2)

    merge.wait_recv()
    second = [ring_copy(bb.at[0, 1], 1, c) for c in range(2)]
    for copy in second:
        copy.start()

    sent = first + second + [mate_own, mate_in, merge]

    def take_end(part):
        for c in range(2):
            end_copy(part, c).wait_recv()

    def take(t):
        for c in range(2):
            ring_copy(bb.at[0, 0], t - 1, c).wait_recv()
            if t <= LAST - 3:
                copy = ring_copy(bb.at[t, c], t + 1, c)
            else:
                copy = end_copy(t - (LAST - 2), c)
            copy.start()
            sent.append(copy)

    def blocks(s):
        if s == 0:
            slots = (0, 0), (0, 1)
        elif s == LAST:
            slots = (LAST, 0), (LAST, 1)
        elif s % 2:
            slots = (s, 0), (s + 1, 0)
        else:
            slots = (s - 1, 1), (s, 1)
        return [lambda slot=slot: bb[slot] for slot in slots]

    def x2_copy(s, part):
        places = pl.ds(part * (NZ // 2), NZ // 2)
        return remote(
            give.at[s, places], x2.at[s, places], x2_send.at[s, part], x2_recv.at[s, part], mate2
        )

    def product(core, rows, mates, right_side):
        own, other = (a_mate.at[0], a_mate.at[1]) if mates else (a_own, a_in)
        lhs = jnp.where(core == k, own[rows], other[rows])
        return jnp.dot(lhs, right_side, preferred_element_type=jnp.float32).reshape(-1, PIECE, TILE)

    GIVEN = ((slice(0, TILE), slice(0, NZ // 2)), (slice(TILE, 2 * TILE), slice(NZ // 2, NZ)))
    KEPT = (slice(0, 2 * TILE), slice(0, NZ))

    def multiply(s):
        mine, mates = blocks(s)
        if s == LAST:
            take_end(0)
            for rows, places in GIVEN:
                give[s, places] = product(1 - s0, rows, False, bb[LAST, 0])
            keep[s] = product(s0, KEPT[0], False, bb[LAST, 0])
            take_end(1)
        for part, (rows, places) in enumerate(GIVEN):
            value = give[s, places] if s == LAST else product(1 - s0, rows, False, mine())
            give[s, places] = value + product(1 - s0, rows, True, mates())
            copy = x2_copy(s, part)
            copy.start()
            sent.append(copy)
        value = keep[s] if s == LAST else product(s0, KEPT[0], False, mine())
        keep[s] = value + product(s0, KEPT[0], True, mates())

    def spread(s):
        for part, (_, places) in enumerate(GIVEN):
            x2_copy(s, part).wait_recv()
            zs[s, places] = keep[s, places] + x2[s, places]
            ways = [(p, (p + 2) % NZ) for p in range(places.start, places.stop)]
            for p, d in sorted(ways, key=lambda way: abs(way[1] - NZ // 2)):
                if d == 0:
                    continue
                remote(
                    zs.at[s, p], zr.at[s, d - 1], z_send.at[s], z_recv.at[s],
                    dev(lax.rem(z + d, NZ), x, y, k),
                ).start()

    def owner(s):
        j = lax.rem(y + NY + (-((s + 1) // 2) if s % 2 else s // 2), NY)
        me = jnp.logical_and(j == z, jnp.logical_and(owner_x == x, s0 == k))
        return j, me

    def deliver(s):
        pltpu.make_async_copy(zr.at[s], zr.at[s], z_recv.at[s]).wait()
        total = zs[s, NZ - 2]
        for d in range(NZ - 1):
            total = total + zr[s, d]
        cv[s] = total.astype(jnp.bfloat16)
        j, me = owner(s)

        @pl.when(me)
        def _():
            copy = pltpu.make_async_copy(cv.at[s], obuf.at[z], load_sem.at[0])
            copy.start()
            copy.wait()

        @pl.when(jnp.logical_not(me))
        def _():
            remote(cv.at[s], obuf.at[z], c_send.at[s], c_recv, dev(j, owner_x, y, s0)).start()

    load_own.wait()
    take(1)
    if LAST > 2:
        take(2)
    hear(2)
    mate_own.wait_recv()
    mate_in.wait_recv()
    for s in range(STEPS + 2):
        if 2 <= s < LAST - 1:
            take(s + 1)
        if s < STEPS:
            multiply(s)
        if 1 <= s < STEPS + 1:
            spread(s - 1)
        if s >= 2:
            deliver(s - 2)

    has_own = jnp.logical_and(owner_x == x, s0 == k)

    @pl.when(has_own)
    def _():
        others = obuf.at[pl.ds(0, NZ - 1)]
        pltpu.make_async_copy(others, others, c_recv).wait()

    @pl.when(jnp.logical_not(has_own))
    def _():
        pltpu.make_async_copy(obuf, obuf, c_recv).wait()

    out_ref[...] = obuf[...].reshape(2 * TILE, TILE)

    for copy in sent:
        copy.wait_send()
    for s in range(STEPS):
        pltpu.make_async_copy(zr.at[s], zr.at[s], z_send.at[s]).wait()
        _, me = owner(s)

        @pl.when(jnp.logical_not(me))
        def _():
            pltpu.make_async_copy(cv.at[s], cv.at[s], c_send.at[s]).wait()


def per_device(tile_values, tile_counts, tile_cols, panels):
    bf16, f32 = jnp.bfloat16, jnp.float32
    dma = pltpu.SemaphoreType.DMA
    depth = panels.shape[0]
    return pl.pallas_call(
        kernel,
        out_shape=jax.ShapeDtypeStruct((2 * TILE, TILE), bf16),
        in_specs=[
            pl.BlockSpec(memory_space=pltpu.SMEM),
            pl.BlockSpec(memory_space=pltpu.SMEM),
            pl.BlockSpec(memory_space=pl.ANY),
            pl.BlockSpec(memory_space=pl.ANY),
        ],
        out_specs=pl.BlockSpec(memory_space=pltpu.VMEM),
        scratch_shapes=[
            pltpu.VMEM(tile_values.shape, bf16),
            pltpu.VMEM((2 * TILE, depth), bf16),
            pltpu.VMEM((2 * TILE, depth), bf16),
            pltpu.VMEM((2, 2 * TILE, depth), bf16),
            pltpu.VMEM((STEPS, 2, depth, TILE), bf16),
            pltpu.VMEM((STEPS, NZ, PIECE, TILE), f32),
            pltpu.VMEM((STEPS, NZ, PIECE, TILE), f32),
            pltpu.VMEM((STEPS, NZ, PIECE, TILE), f32),
            pltpu.VMEM((STEPS, NZ, PIECE, TILE), f32),
            pltpu.VMEM((STEPS, NZ - 1, PIECE, TILE), f32),
            pltpu.VMEM((STEPS, PIECE, TILE), bf16),
            pltpu.VMEM((NZ, PIECE, TILE), bf16),
            dma((2,)), dma, dma,
            dma((STEPS, 2)), dma((STEPS, 2)), dma((2, 2)), dma((2, 2)), dma((3,)), dma((3,)),
            dma((STEPS, 2)), dma((STEPS, 2)), dma((STEPS,)), dma((STEPS,)), dma((STEPS,)), dma,
            pltpu.SemaphoreType.REGULAR((3, 2)),
        ],
        compiler_params=pltpu.CompilerParams(
            collective_id=0, has_side_effects=True, vmem_limit_bytes=55000 * 1024
        ),
    )(tile_counts.T, tile_cols.T, tile_values, panels)


def solution(mesh):
    return jax.shard_map(
        per_device,
        mesh=mesh,
        in_specs=(P("row", "col", None), P("row", "col"), P("row", "col"), P("row", "col")),
        out_specs=P("col", "row"),
        check_vma=False,
    )
```

```python
import jax
import jax.numpy as jnp
from jax import lax
from jax.experimental import pallas as pl
from jax.experimental.pallas import tpu as pltpu
from jax.sharding import PartitionSpec as P

MESH = pl.DeviceIdType.MESH
NX, NZ, NY = 4, 8, 8
TILE = 128
STEPS = NY
LAST = STEPS - 1
PIECE = 2 * TILE // NZ


def kernel(
    counts_any, cols_any, tv_hbm, p_hbm, out_ref,
    counts, cols, tvb, a_own, a_in, a_mate, bb, give, keep, x2, zs, zr, cv, obuf,
    load_sem, a_send, a_recv, b_send, b_recv, e_send, e_recv, m_send, m_recv,
    x2_send, x2_recv, z_send, z_recv, c_send, c_recv, known,
):
    row, col = lax.axis_index("row"), lax.axis_index("col")
    z, x = row // NX, lax.rem(row, NX)
    y, k = col // 2, lax.rem(col, 2)
    depth = p_hbm.shape[0]
    half_depth = depth // 2

    def dev(z_, x_, y_, k_):
        return (z_ * NX + x_, y_ * 2 + k_)

    right = dev(z, x, lax.rem(y + 1, NY), k)
    left = dev(z, x, lax.rem(y + NY - 1, NY), k)
    above = dev(lax.rem(z + 1, NZ), x, y, k)
    below = dev(lax.rem(z + NZ - 1, NZ), x, y, k)
    sibling = dev(z, x, y, 1 - k)
    flip = x + 1 - 2 * lax.rem(x, 2)
    bit1 = x // 2
    bit0 = lax.rem(bit1 + x, 2)
    swap = k * (NX - 1 - x - flip)
    turn_bit = k * (bit1 - bit0)
    s1, s0 = bit0 + turn_bit, bit1 - turn_bit
    mate1 = dev(z, flip + swap, y, k)
    mate2 = dev(z, NX - 1 - x - swap, y, k)
    owner_x = 2 * k + s1

    def remote(src, dst, send, recv, to):
        return pltpu.make_async_remote_copy(
            src_ref=src, dst_ref=dst, send_sem=send, recv_sem=recv,
            device_id=to, device_id_type=MESH,
        )

    barrier = pltpu.get_barrier_semaphore()
    peers = [right, left, sibling, mate1, mate2, above, below]
    for peer in peers:
        pl.semaphore_signal(barrier, inc=1, device_id=peer, device_id_type=MESH)

    load_tiles = pltpu.make_async_copy(tv_hbm, tvb, load_sem.at[0])
    load_tiles.start()
    load_counts = pltpu.make_async_copy(counts_any, counts, load_sem.at[2])
    load_counts.start()
    load_cols = pltpu.make_async_copy(cols_any, cols, load_sem.at[3])
    load_cols.start()
    own_columns = p_hbm.at[:, pl.ds(pl.multiple_of(s1 * TILE, TILE), TILE)]
    mate_columns = p_hbm.at[:, pl.ds(pl.multiple_of((1 - s1) * TILE, TILE), TILE)]
    load_own = pltpu.make_async_copy(own_columns, bb.at[0, 0], load_sem.at[1])
    load_own.start()

    pl.semaphore_wait(barrier, len(peers))

    def tell(r):
        for side, peer in ((0, above), (1, below)):
            pl.semaphore_signal(known.at[r, side], inc=1, device_id=peer, device_id_type=MESH)

    def hear(r):
        for side in range(2):
            pl.semaphore_wait(known.at[r, side], 1)

    def ring_copy(src, i, c):
        return remote(src, bb.at[i + 1, c], b_send.at[i, c], b_recv.at[i + 1, c], left if c else right)

    def end_copy(part, c):
        rows = pl.ds(c * half_depth, half_depth)
        src = bb.at[LAST - 2 + part, c, rows]
        return remote(src, bb.at[LAST, part, rows], e_send.at[part, c], e_recv.at[part, c], left if c else right)

    first = [ring_copy(own_columns, 0, c) for c in range(2)]
    for copy in first:
        copy.start()
    merge = remote(mate_columns, bb.at[0, 1], m_send.at[2], m_recv.at[2], mate1)
    merge.start()
    tell(0)

    load_tiles.wait()
    load_counts.wait()
    load_cols.wait()

    def build(i, start):
        n = counts[0, i]
        for b in range(2):
            slot = jnp.minimum(start + jnp.where(n == 2, b, 0), cols.shape[1] - 1)
            valid = jnp.logical_or(n == 2, jnp.logical_and(n == 1, cols[0, slot] == b))
            tile = tvb[slot].T
            tile = jnp.where(valid, tile, jnp.zeros_like(tile))
            for q in range(TILE // PIECE):
                place = lax.rem(b * (TILE // PIECE) + q - z + 2 * NZ - 2, NZ)
                rows = pl.ds(pl.multiple_of(place * PIECE, PIECE), PIECE)
                lanes = pl.ds(pl.multiple_of(i * TILE, TILE), TILE)
                a_own[rows, lanes] = tile[q * PIECE:(q + 1) * PIECE]
        return start + n

    lax.fori_loop(0, counts.shape[1], build, jnp.int32(0))
    a_copy = remote(a_own, a_in, a_send, a_recv, sibling)
    a_copy.start()
    mate_own = remote(a_own, a_mate.at[0], m_send.at[0], m_recv.at[0], mate1)
    mate_own.start()
    hear(0)
    tell(1)
    a_copy.wait()
    mate_in = remote(a_in, a_mate.at[1], m_send.at[1], m_recv.at[1], mate1)
    mate_in.start()
    hear(1)
    tell(2)

    merge.wait_recv()
    second = [ring_copy(bb.at[0, 1], 1, c) for c in range(2)]
    for copy in second:
        copy.start()

    sent = first + second + [mate_own, mate_in, merge]

    def take_end(part):
        for c in range(2):
            end_copy(part, c).wait_recv()

    def take(t):
        for c in range(2):
            ring_copy(bb.at[0, 0], t - 1, c).wait_recv()
            if t <= LAST - 3:
                copy = ring_copy(bb.at[t, c], t + 1, c)
            else:
                copy = end_copy(t - (LAST - 2), c)
            copy.start()
            sent.append(copy)

    def blocks(s):
        if s == 0:
            slots = (0, 0), (0, 1)
        elif s == LAST:
            slots = (LAST, 0), (LAST, 1)
        elif s % 2:
            slots = (s, 0), (s + 1, 0)
        else:
            slots = (s - 1, 1), (s, 1)
        return [lambda slot=slot: bb[slot] for slot in slots]

    def x2_copy(s, part):
        places = pl.ds(part * (NZ // 2), NZ // 2)
        return remote(
            give.at[s, places], x2.at[s, places], x2_send.at[s, part], x2_recv.at[s, part], mate2
        )

    def product(core, rows, mates, right_side):
        own, other = (a_mate.at[0], a_mate.at[1]) if mates else (a_own, a_in)
        lhs = jnp.where(core == k, own[rows], other[rows])
        return jnp.dot(lhs, right_side, preferred_element_type=jnp.float32).reshape(-1, PIECE, TILE)

    GIVEN = ((slice(0, TILE), slice(0, NZ // 2)), (slice(TILE, 2 * TILE), slice(NZ // 2, NZ)))
    KEPT = (slice(0, 2 * TILE), slice(0, NZ))

    def multiply(s):
        mine, mates = blocks(s)
        if s == LAST:
            take_end(0)
            for rows, places in GIVEN:
                give[s, places] = product(1 - s0, rows, False, bb[LAST, 0])
            keep[s] = product(s0, KEPT[0], False, bb[LAST, 0])
            take_end(1)
        for part, (rows, places) in enumerate(GIVEN):
            value = give[s, places] if s == LAST else product(1 - s0, rows, False, mine())
            give[s, places] = value + product(1 - s0, rows, True, mates())
            copy = x2_copy(s, part)
            copy.start()
            sent.append(copy)
        value = keep[s] if s == LAST else product(s0, KEPT[0], False, mine())
        keep[s] = value + product(s0, KEPT[0], True, mates())

    def spread(s):
        for part, (_, places) in enumerate(GIVEN):
            x2_copy(s, part).wait_recv()
            zs[s, places] = keep[s, places] + x2[s, places]
            ways = [(p, (p + 2) % NZ) for p in range(places.start, places.stop)]
            for p, d in sorted(ways, key=lambda way: abs(way[1] - NZ // 2)):
                if d == 0:
                    continue
                remote(
                    zs.at[s, p], zr.at[s, d - 1], z_send.at[s], z_recv.at[s],
                    dev(lax.rem(z + d, NZ), x, y, k),
                ).start()

    def owner(s):
        j = lax.rem(y + NY + (-((s + 1) // 2) if s % 2 else s // 2), NY)
        me = jnp.logical_and(j == z, jnp.logical_and(owner_x == x, s0 == k))
        return j, me

    def deliver(s):
        pltpu.make_async_copy(zr.at[s], zr.at[s], z_recv.at[s]).wait()
        total = zs[s, NZ - 2]
        for d in range(NZ - 1):
            total = total + zr[s, d]
        cv[s] = total.astype(jnp.bfloat16)
        j, me = owner(s)

        @pl.when(me)
        def _():
            copy = pltpu.make_async_copy(cv.at[s], obuf.at[z], load_sem.at[0])
            copy.start()
            copy.wait()

        @pl.when(jnp.logical_not(me))
        def _():
            remote(cv.at[s], obuf.at[z], c_send.at[s], c_recv, dev(j, owner_x, y, s0)).start()

    load_own.wait()
    take(1)
    if LAST > 2:
        take(2)
    hear(2)
    mate_own.wait_recv()
    mate_in.wait_recv()
    for s in range(STEPS + 2):
        if 2 <= s < LAST - 1:
            take(s + 1)
        if s < STEPS:
            multiply(s)
        if 1 <= s < STEPS + 1:
            spread(s - 1)
        if s >= 2:
            deliver(s - 2)

    has_own = jnp.logical_and(owner_x == x, s0 == k)

    @pl.when(has_own)
    def _():
        others = obuf.at[pl.ds(0, NZ - 1)]
        pltpu.make_async_copy(others, others, c_recv).wait()

    @pl.when(jnp.logical_not(has_own))
    def _():
        pltpu.make_async_copy(obuf, obuf, c_recv).wait()

    out_ref[...] = obuf[...].reshape(2 * TILE, TILE)

    for copy in sent:
        copy.wait_send()
    for s in range(STEPS):
        pltpu.make_async_copy(zr.at[s], zr.at[s], z_send.at[s]).wait()
        _, me = owner(s)

        @pl.when(jnp.logical_not(me))
        def _():
            pltpu.make_async_copy(cv.at[s], cv.at[s], c_send.at[s]).wait()


def per_device(tile_values, tile_counts, tile_cols, panels):
    bf16, f32 = jnp.bfloat16, jnp.float32
    dma = pltpu.SemaphoreType.DMA
    depth = panels.shape[0]
    return pl.pallas_call(
        kernel,
        out_shape=jax.ShapeDtypeStruct((2 * TILE, TILE), bf16),
        in_specs=[
            pl.BlockSpec(memory_space=pl.ANY),
            pl.BlockSpec(memory_space=pl.ANY),
            pl.BlockSpec(memory_space=pl.ANY),
            pl.BlockSpec(memory_space=pl.ANY),
        ],
        out_specs=pl.BlockSpec(memory_space=pltpu.VMEM),
        scratch_shapes=[
            pltpu.SMEM((1, tile_counts.shape[0]), jnp.int32),
            pltpu.SMEM((1, tile_cols.shape[0]), jnp.int32),
            pltpu.VMEM(tile_values.shape, bf16),
            pltpu.VMEM((2 * TILE, depth), bf16),
            pltpu.VMEM((2 * TILE, depth), bf16),
            pltpu.VMEM((2, 2 * TILE, depth), bf16),
            pltpu.VMEM((STEPS, 2, depth, TILE), bf16),
            pltpu.VMEM((STEPS, NZ, PIECE, TILE), f32),
            pltpu.VMEM((STEPS, NZ, PIECE, TILE), f32),
            pltpu.VMEM((STEPS, NZ, PIECE, TILE), f32),
            pltpu.VMEM((STEPS, NZ, PIECE, TILE), f32),
            pltpu.VMEM((STEPS, NZ - 1, PIECE, TILE), f32),
            pltpu.VMEM((STEPS, PIECE, TILE), bf16),
            pltpu.VMEM((NZ, PIECE, TILE), bf16),
            dma((4,)), dma, dma,
            dma((STEPS, 2)), dma((STEPS, 2)), dma((2, 2)), dma((2, 2)), dma((3,)), dma((3,)),
            dma((STEPS, 2)), dma((STEPS, 2)), dma((STEPS,)), dma((STEPS,)), dma((STEPS,)), dma,
            pltpu.SemaphoreType.REGULAR((3, 2)),
        ],
        compiler_params=pltpu.CompilerParams(
            collective_id=0, has_side_effects=True, vmem_limit_bytes=55000 * 1024
        ),
    )(tile_counts.T, tile_cols.T, tile_values, panels)


def solution(mesh):
    return jax.shard_map(
        per_device,
        mesh=mesh,
        in_specs=(P("row", "col", None), P("row", "col"), P("row", "col"), P("row", "col")),
        out_specs=P("col", "row"),
        check_vma=False,
    )
```

```python
import jax
import jax.numpy as jnp
from jax import lax
from jax.experimental import pallas as pl
from jax.experimental.pallas import tpu as pltpu
from jax.sharding import PartitionSpec as P

MESH = pl.DeviceIdType.MESH
NX, NZ, NY = 4, 8, 8
TILE = 128
STEPS = NY
LAST = STEPS - 1
PIECE = 2 * TILE // NZ


def kernel(
    counts_any, cols_any, tv_hbm, p_hbm, out_ref,
    counts, cols, tvb, a_own, a_in, a_mate, bb, give, keep, x2, zs, zr, cv, obuf,
    load_sem, a_send, a_recv, b_send, b_recv, e_send, e_recv, m_send, m_recv,
    x2_send, x2_recv, z_send, z_recv, c_send, c_recv, known,
):
    row, col = lax.axis_index("row"), lax.axis_index("col")
    z, x = row // NX, lax.rem(row, NX)
    y, k = col // 2, lax.rem(col, 2)
    depth = p_hbm.shape[0]
    half_depth = depth // 2

    def dev(z_, x_, y_, k_):
        return (z_ * NX + x_, y_ * 2 + k_)

    right = dev(z, x, lax.rem(y + 1, NY), k)
    left = dev(z, x, lax.rem(y + NY - 1, NY), k)
    above = dev(lax.rem(z + 1, NZ), x, y, k)
    below = dev(lax.rem(z + NZ - 1, NZ), x, y, k)
    sibling = dev(z, x, y, 1 - k)
    flip = x + 1 - 2 * lax.rem(x, 2)
    bit1 = x // 2
    bit0 = lax.rem(bit1 + x, 2)
    swap = (1 - k) * (NX - 1 - x - flip)
    turn_bit = (1 - k) * (bit1 - bit0)
    s1, s0 = bit0 + turn_bit, bit1 - turn_bit
    mate1 = dev(z, flip + swap, y, k)
    mate2 = dev(z, NX - 1 - x - swap, y, k)
    owner_x = 2 * k + s1

    def remote(src, dst, send, recv, to):
        return pltpu.make_async_remote_copy(
            src_ref=src, dst_ref=dst, send_sem=send, recv_sem=recv,
            device_id=to, device_id_type=MESH,
        )

    barrier = pltpu.get_barrier_semaphore()
    peers = [right, left, sibling, mate1, mate2, above, below]
    for peer in peers:
        pl.semaphore_signal(barrier, inc=1, device_id=peer, device_id_type=MESH)

    load_tiles = pltpu.make_async_copy(tv_hbm, tvb, load_sem.at[0])
    load_tiles.start()
    load_counts = pltpu.make_async_copy(counts_any, counts, load_sem.at[2])
    load_counts.start()
    load_cols = pltpu.make_async_copy(cols_any, cols, load_sem.at[3])
    load_cols.start()
    own_columns = p_hbm.at[:, pl.ds(pl.multiple_of(s1 * TILE, TILE), TILE)]
    mate_columns = p_hbm.at[:, pl.ds(pl.multiple_of((1 - s1) * TILE, TILE), TILE)]
    load_own = pltpu.make_async_copy(own_columns, bb.at[0, 0], load_sem.at[1])
    load_own.start()

    pl.semaphore_wait(barrier, len(peers))

    def tell(r):
        for side, peer in ((0, above), (1, below)):
            pl.semaphore_signal(known.at[r, side], inc=1, device_id=peer, device_id_type=MESH)

    def hear(r):
        for side in range(2):
            pl.semaphore_wait(known.at[r, side], 1)

    def ring_copy(src, i, c):
        return remote(src, bb.at[i + 1, c], b_send.at[i, c], b_recv.at[i + 1, c], left if c else right)

    def end_copy(part, c):
        rows = pl.ds(c * half_depth, half_depth)
        src = bb.at[LAST - 2 + part, c, rows]
        return remote(src, bb.at[LAST, part, rows], e_send.at[part, c], e_recv.at[part, c], left if c else right)

    first = [ring_copy(own_columns, 0, c) for c in range(2)]
    for copy in first:
        copy.start()
    merge = remote(mate_columns, bb.at[0, 1], m_send.at[2], m_recv.at[2], mate1)
    merge.start()
    tell(0)

    load_tiles.wait()
    load_counts.wait()
    load_cols.wait()

    def build(i, start):
        n = counts[0, i]
        for b in range(2):
            slot = jnp.minimum(start + jnp.where(n == 2, b, 0), cols.shape[1] - 1)
            valid = jnp.logical_or(n == 2, jnp.logical_and(n == 1, cols[0, slot] == b))
            tile = tvb[slot].T
            tile = jnp.where(valid, tile, jnp.zeros_like(tile))
            for q in range(TILE // PIECE):
                place = lax.rem(b * (TILE // PIECE) + q - z + 2 * NZ - 2, NZ)
                rows = pl.ds(pl.multiple_of(place * PIECE, PIECE), PIECE)
                lanes = pl.ds(pl.multiple_of(i * TILE, TILE), TILE)
                a_own[rows, lanes] = tile[q * PIECE:(q + 1) * PIECE]
        return start + n

    lax.fori_loop(0, counts.shape[1], build, jnp.int32(0))
    a_copy = remote(a_own, a_in, a_send, a_recv, sibling)
    a_copy.start()
    mate_own = remote(a_own, a_mate.at[0], m_send.at[0], m_recv.at[0], mate1)
    mate_own.start()
    hear(0)
    tell(1)
    a_copy.wait()
    mate_in = remote(a_in, a_mate.at[1], m_send.at[1], m_recv.at[1], mate1)
    mate_in.start()
    hear(1)
    tell(2)

    merge.wait_recv()
    second = [ring_copy(bb.at[0, 1], 1, c) for c in range(2)]
    for copy in second:
        copy.start()

    sent = first + second + [mate_own, mate_in, merge]

    def take_end(part):
        for c in range(2):
            end_copy(part, c).wait_recv()

    def take(t):
        for c in range(2):
            ring_copy(bb.at[0, 0], t - 1, c).wait_recv()
            if t <= LAST - 3:
                copy = ring_copy(bb.at[t, c], t + 1, c)
            else:
                copy = end_copy(t - (LAST - 2), c)
            copy.start()
            sent.append(copy)

    def blocks(s):
        if s == 0:
            slots = (0, 0), (0, 1)
        elif s == LAST:
            slots = (LAST, 0), (LAST, 1)
        elif s % 2:
            slots = (s, 0), (s + 1, 0)
        else:
            slots = (s - 1, 1), (s, 1)
        return [lambda slot=slot: bb[slot] for slot in slots]

    def x2_copy(s, part):
        places = pl.ds(part * (NZ // 2), NZ // 2)
        return remote(
            give.at[s, places], x2.at[s, places], x2_send.at[s, part], x2_recv.at[s, part], mate2
        )

    def product(core, rows, mates, right_side):
        own, other = (a_mate.at[0], a_mate.at[1]) if mates else (a_own, a_in)
        lhs = jnp.where(core == k, own[rows], other[rows])
        return jnp.dot(lhs, right_side, preferred_element_type=jnp.float32).reshape(-1, PIECE, TILE)

    GIVEN = ((slice(0, TILE), slice(0, NZ // 2)), (slice(TILE, 2 * TILE), slice(NZ // 2, NZ)))
    KEPT = (slice(0, 2 * TILE), slice(0, NZ))

    def ahead(s):
        mine, _ = blocks(s)
        for rows, places in GIVEN:
            give[s, places] = product(1 - s0, rows, False, mine())
        keep[s] = product(s0, KEPT[0], False, mine())

    def multiply(s):
        mine, mates = blocks(s)
        for part, (rows, places) in enumerate(GIVEN):
            value = give[s, places] if s >= LAST - 2 else product(1 - s0, rows, False, mine())
            give[s, places] = value + product(1 - s0, rows, True, mates())
            copy = x2_copy(s, part)
            copy.start()
            sent.append(copy)
        value = keep[s] if s >= LAST - 2 else product(s0, KEPT[0], False, mine())
        keep[s] = value + product(s0, KEPT[0], True, mates())

    def spread(s):
        for part, (_, places) in enumerate(GIVEN):
            x2_copy(s, part).wait_recv()
            zs[s, places] = keep[s, places] + x2[s, places]
            ways = [(p, (p + 2) % NZ) for p in range(places.start, places.stop)]
            for p, d in sorted(ways, key=lambda way: abs(way[1] - NZ // 2)):
                if d == 0:
                    continue
                remote(
                    zs.at[s, p], zr.at[s, d - 1], z_send.at[s], z_recv.at[s],
                    dev(lax.rem(z + d, NZ), x, y, k),
                ).start()

    def owner(s):
        j = lax.rem(y + NY + (-((s + 1) // 2) if s % 2 else s // 2), NY)
        me = jnp.logical_and(j == z, jnp.logical_and(owner_x == x, s0 == k))
        return j, me

    def deliver(s):
        pltpu.make_async_copy(zr.at[s], zr.at[s], z_recv.at[s]).wait()
        total = zs[s, NZ - 2]
        for d in range(NZ - 1):
            total = total + zr[s, d]
        cv[s] = total.astype(jnp.bfloat16)
        j, me = owner(s)

        @pl.when(me)
        def _():
            copy = pltpu.make_async_copy(cv.at[s], obuf.at[z], load_sem.at[0])
            copy.start()
            copy.wait()

        @pl.when(jnp.logical_not(me))
        def _():
            remote(cv.at[s], obuf.at[z], c_send.at[s], c_recv, dev(j, owner_x, y, s0)).start()

    load_own.wait()
    take(1)
    if LAST > 2:
        take(2)
    hear(2)
    mate_own.wait_recv()
    mate_in.wait_recv()
    for s in range(STEPS + 2):
        if 2 <= s < LAST - 1:
            take(s + 1)
        if s == LAST:
            take_end(0)
            ahead(LAST)
            spread(LAST - 1)
            take_end(1)
        if s < STEPS:
            multiply(s)
        if 1 <= s < STEPS + 1 and s != LAST:
            spread(s - 1)
        if s >= 2:
            deliver(s - 2)
        if s == LAST - 3:
            ahead(LAST - 2)
            ahead(LAST - 1)

    has_own = jnp.logical_and(owner_x == x, s0 == k)

    @pl.when(has_own)
    def _():
        others = obuf.at[pl.ds(0, NZ - 1)]
        pltpu.make_async_copy(others, others, c_recv).wait()

    @pl.when(jnp.logical_not(has_own))
    def _():
        pltpu.make_async_copy(obuf, obuf, c_recv).wait()

    out_ref[...] = obuf[...].reshape(2 * TILE, TILE)

    for copy in sent:
        copy.wait_send()
    for s in range(STEPS):
        pltpu.make_async_copy(zr.at[s], zr.at[s], z_send.at[s]).wait()
        _, me = owner(s)

        @pl.when(jnp.logical_not(me))
        def _():
            pltpu.make_async_copy(cv.at[s], cv.at[s], c_send.at[s]).wait()


def per_device(tile_values, tile_counts, tile_cols, panels):
    bf16, f32 = jnp.bfloat16, jnp.float32
    dma = pltpu.SemaphoreType.DMA
    depth = panels.shape[0]
    return pl.pallas_call(
        kernel,
        out_shape=jax.ShapeDtypeStruct((2 * TILE, TILE), bf16),
        in_specs=[
            pl.BlockSpec(memory_space=pl.ANY),
            pl.BlockSpec(memory_space=pl.ANY),
            pl.BlockSpec(memory_space=pl.ANY),
            pl.BlockSpec(memory_space=pl.ANY),
        ],
        out_specs=pl.BlockSpec(memory_space=pltpu.VMEM),
        scratch_shapes=[
            pltpu.SMEM((1, tile_counts.shape[0]), jnp.int32),
            pltpu.SMEM((1, tile_cols.shape[0]), jnp.int32),
            pltpu.VMEM(tile_values.shape, bf16),
            pltpu.VMEM((2 * TILE, depth), bf16),
            pltpu.VMEM((2 * TILE, depth), bf16),
            pltpu.VMEM((2, 2 * TILE, depth), bf16),
            pltpu.VMEM((STEPS, 2, depth, TILE), bf16),
            pltpu.VMEM((STEPS, NZ, PIECE, TILE), f32),
            pltpu.VMEM((STEPS, NZ, PIECE, TILE), f32),
            pltpu.VMEM((STEPS, NZ, PIECE, TILE), f32),
            pltpu.VMEM((STEPS, NZ, PIECE, TILE), f32),
            pltpu.VMEM((STEPS, NZ - 1, PIECE, TILE), f32),
            pltpu.VMEM((STEPS, PIECE, TILE), bf16),
            pltpu.VMEM((NZ, PIECE, TILE), bf16),
            dma((4,)), dma, dma,
            dma((STEPS, 2)), dma((STEPS, 2)), dma((2, 2)), dma((2, 2)), dma((3,)), dma((3,)),
            dma((STEPS, 2)), dma((STEPS, 2)), dma((STEPS,)), dma((STEPS,)), dma((STEPS,)), dma,
            pltpu.SemaphoreType.REGULAR((3, 2)),
        ],
        compiler_params=pltpu.CompilerParams(
            collective_id=0, has_side_effects=True, vmem_limit_bytes=55000 * 1024
        ),
    )(tile_counts.T, tile_cols.T, tile_values, panels)


def solution(mesh):
    return jax.shard_map(
        per_device,
        mesh=mesh,
        in_specs=(P("row", "col", None), P("row", "col"), P("row", "col"), P("row", "col")),
        out_specs=P("col", "row"),
        check_vma=False,
    )
```

```python
import jax
import jax.numpy as jnp
from jax import lax
from jax.experimental import pallas as pl
from jax.experimental.pallas import tpu as pltpu
from jax.sharding import PartitionSpec as P

MESH = pl.DeviceIdType.MESH
NX, NZ, NY = 4, 8, 8
TILE = 128
STEPS = NY
LAST = STEPS - 1
PIECE = 2 * TILE // NZ


def kernel(
    counts_any, cols_any, tv_hbm, p_hbm, out_ref,
    counts, cols, tvb, a_own, a_in, a_mate, bb, give, keep, x2, zs, zr, cv,
    load_sem, a_send, a_recv, b_send, b_recv, e_send, e_recv, m_send, m_recv,
    x2_send, x2_recv, z_send, z_recv, c_send, c_recv, known,
):
    row, col = lax.axis_index("row"), lax.axis_index("col")
    z, x = row // NX, lax.rem(row, NX)
    y, k = col // 2, lax.rem(col, 2)
    depth = p_hbm.shape[0]
    half_depth = depth // 2

    def dev(z_, x_, y_, k_):
        return (z_ * NX + x_, y_ * 2 + k_)

    right = dev(z, x, lax.rem(y + 1, NY), k)
    left = dev(z, x, lax.rem(y + NY - 1, NY), k)
    above = dev(lax.rem(z + 1, NZ), x, y, k)
    below = dev(lax.rem(z + NZ - 1, NZ), x, y, k)
    sibling = dev(z, x, y, 1 - k)
    flip = x + 1 - 2 * lax.rem(x, 2)
    bit1 = x // 2
    bit0 = lax.rem(bit1 + x, 2)
    swap = (1 - k) * (NX - 1 - x - flip)
    turn_bit = (1 - k) * (bit1 - bit0)
    s1, s0 = bit0 + turn_bit, bit1 - turn_bit
    mate1 = dev(z, flip + swap, y, k)
    mate2 = dev(z, NX - 1 - x - swap, y, k)
    owner_x = 2 * k + s1

    def remote(src, dst, send, recv, to):
        return pltpu.make_async_remote_copy(
            src_ref=src, dst_ref=dst, send_sem=send, recv_sem=recv,
            device_id=to, device_id_type=MESH,
        )

    barrier = pltpu.get_barrier_semaphore()
    peers = [right, left, sibling, mate1, mate2, above, below]
    for peer in peers:
        pl.semaphore_signal(barrier, inc=1, device_id=peer, device_id_type=MESH)

    load_tiles = pltpu.make_async_copy(tv_hbm, tvb, load_sem.at[0])
    load_tiles.start()
    load_counts = pltpu.make_async_copy(counts_any, counts, load_sem.at[2])
    load_counts.start()
    load_cols = pltpu.make_async_copy(cols_any, cols, load_sem.at[3])
    load_cols.start()
    own_columns = p_hbm.at[:, pl.ds(pl.multiple_of(s1 * TILE, TILE), TILE)]
    mate_columns = p_hbm.at[:, pl.ds(pl.multiple_of((1 - s1) * TILE, TILE), TILE)]
    load_own = pltpu.make_async_copy(own_columns, bb.at[0, 0], load_sem.at[1])
    load_own.start()

    pl.semaphore_wait(barrier, len(peers))

    def tell(r):
        for side, peer in ((0, above), (1, below)):
            pl.semaphore_signal(known.at[r, side], inc=1, device_id=peer, device_id_type=MESH)

    def hear(r):
        for side in range(2):
            pl.semaphore_wait(known.at[r, side], 1)

    def ring_copy(src, i, c):
        return remote(src, bb.at[i + 1, c], b_send.at[i, c], b_recv.at[i + 1, c], left if c else right)

    def end_copy(part, c):
        rows = pl.ds(c * half_depth, half_depth)
        src = bb.at[LAST - 2 + part, c, rows]
        return remote(src, bb.at[LAST, part, rows], e_send.at[part, c], e_recv.at[part, c], left if c else right)

    first = [ring_copy(own_columns, 0, c) for c in range(2)]
    for copy in first:
        copy.start()
    merge = remote(mate_columns, bb.at[0, 1], m_send.at[2], m_recv.at[2], mate1)
    merge.start()
    tell(0)

    load_tiles.wait()
    load_counts.wait()
    load_cols.wait()

    def build(i, start):
        n = counts[0, i]
        for b in range(2):
            slot = jnp.minimum(start + jnp.where(n == 2, b, 0), cols.shape[1] - 1)
            valid = jnp.logical_or(n == 2, jnp.logical_and(n == 1, cols[0, slot] == b))
            tile = tvb[slot].T
            tile = jnp.where(valid, tile, jnp.zeros_like(tile))
            for q in range(TILE // PIECE):
                place = lax.rem(b * (TILE // PIECE) + q - z + 2 * NZ - 2, NZ)
                rows = pl.ds(pl.multiple_of(place * PIECE, PIECE), PIECE)
                lanes = pl.ds(pl.multiple_of(i * TILE, TILE), TILE)
                a_own[rows, lanes] = tile[q * PIECE:(q + 1) * PIECE]
        return start + n

    lax.fori_loop(0, counts.shape[1], build, jnp.int32(0))
    a_copy = remote(a_own, a_in, a_send, a_recv, sibling)
    a_copy.start()
    mate_own = remote(a_own, a_mate.at[0], m_send.at[0], m_recv.at[0], mate1)
    mate_own.start()
    hear(0)
    tell(1)
    a_copy.wait()
    mate_in = remote(a_in, a_mate.at[1], m_send.at[1], m_recv.at[1], mate1)
    mate_in.start()
    hear(1)
    tell(2)

    merge.wait_recv()
    second = [ring_copy(bb.at[0, 1], 1, c) for c in range(2)]
    for copy in second:
        copy.start()

    sent = first + second + [mate_own, mate_in, merge]

    def take_end(part):
        for c in range(2):
            end_copy(part, c).wait_recv()

    def take(t):
        for c in range(2):
            ring_copy(bb.at[0, 0], t - 1, c).wait_recv()
            if t <= LAST - 3:
                copy = ring_copy(bb.at[t, c], t + 1, c)
            else:
                copy = end_copy(t - (LAST - 2), c)
            copy.start()
            sent.append(copy)

    def blocks(s):
        if s == 0:
            slots = (0, 0), (0, 1)
        elif s == LAST:
            slots = (LAST, 0), (LAST, 1)
        elif s % 2:
            slots = (s, 0), (s + 1, 0)
        else:
            slots = (s - 1, 1), (s, 1)
        return [lambda slot=slot: bb[slot] for slot in slots]

    def x2_copy(s, part):
        places = pl.ds(part * (NZ // 2), NZ // 2)
        return remote(
            give.at[s, places], x2.at[s, places], x2_send.at[s, part], x2_recv.at[s, part], mate2
        )

    def product(core, rows, mates, right_side):
        own, other = (a_mate.at[0], a_mate.at[1]) if mates else (a_own, a_in)
        lhs = jnp.where(core == k, own[rows], other[rows])
        return jnp.dot(lhs, right_side, preferred_element_type=jnp.float32).reshape(-1, PIECE, TILE)

    GIVEN = ((slice(0, TILE), slice(0, NZ // 2)), (slice(TILE, 2 * TILE), slice(NZ // 2, NZ)))
    KEPT = (slice(0, 2 * TILE), slice(0, NZ))

    def ahead(s):
        mine, _ = blocks(s)
        for rows, places in GIVEN:
            give[s, places] = product(1 - s0, rows, False, mine())
        keep[s] = product(s0, KEPT[0], False, mine())

    def multiply(s):
        mine, mates = blocks(s)
        for part, (rows, places) in enumerate(GIVEN):
            value = give[s, places] if s >= LAST - 2 else product(1 - s0, rows, False, mine())
            give[s, places] = value + product(1 - s0, rows, True, mates())
            copy = x2_copy(s, part)
            copy.start()
            sent.append(copy)
        value = keep[s] if s >= LAST - 2 else product(s0, KEPT[0], False, mine())
        keep[s] = value + product(s0, KEPT[0], True, mates())

    def spread(s):
        for part, (_, places) in enumerate(GIVEN):
            x2_copy(s, part).wait_recv()
            zs[s, places] = keep[s, places] + x2[s, places]
            ways = [(p, (p + 2) % NZ) for p in range(places.start, places.stop)]
            for p, d in sorted(ways, key=lambda way: abs(way[1] - NZ // 2)):
                if d == 0:
                    continue
                remote(
                    zs.at[s, p], zr.at[s, d - 1], z_send.at[s], z_recv.at[s],
                    dev(lax.rem(z + d, NZ), x, y, k),
                ).start()

    def owner(s):
        j = lax.rem(y + NY + (-((s + 1) // 2) if s % 2 else s // 2), NY)
        me = jnp.logical_and(j == z, jnp.logical_and(owner_x == x, s0 == k))
        return j, me

    def deliver(s):
        pltpu.make_async_copy(zr.at[s], zr.at[s], z_recv.at[s]).wait()
        total = zs[s, NZ - 2]
        for d in range(NZ - 1):
            total = total + zr[s, d]
        cv[s] = total.astype(jnp.bfloat16)
        j, me = owner(s)

        @pl.when(me)
        def _():
            copy = pltpu.make_async_copy(cv.at[s], out_ref.at[pl.ds(z * PIECE, PIECE)], load_sem.at[0])
            copy.start()
            copy.wait()

        @pl.when(jnp.logical_not(me))
        def _():
            remote(cv.at[s], out_ref.at[pl.ds(z * PIECE, PIECE)], c_send.at[s], c_recv, dev(j, owner_x, y, s0)).start()

    load_own.wait()
    take(1)
    if LAST > 2:
        take(2)
    hear(2)
    mate_own.wait_recv()
    mate_in.wait_recv()
    for s in range(STEPS + 2):
        if 2 <= s < LAST - 1:
            take(s + 1)
        if s == LAST:
            take_end(0)
            ahead(LAST)
            spread(LAST - 1)
            take_end(1)
        if s < STEPS:
            multiply(s)
        if 1 <= s < STEPS + 1 and s != LAST:
            spread(s - 1)
        if s >= 2:
            deliver(s - 2)
        if s == LAST - 3:
            ahead(LAST - 2)
            ahead(LAST - 1)

    has_own = jnp.logical_and(owner_x == x, s0 == k)

    @pl.when(has_own)
    def _():
        others = out_ref.at[pl.ds(0, (NZ - 1) * PIECE)]
        pltpu.make_async_copy(others, others, c_recv).wait()

    @pl.when(jnp.logical_not(has_own))
    def _():
        pltpu.make_async_copy(out_ref, out_ref, c_recv).wait()

    for copy in sent:
        copy.wait_send()
    for s in range(STEPS):
        pltpu.make_async_copy(zr.at[s], zr.at[s], z_send.at[s]).wait()
        _, me = owner(s)

        @pl.when(jnp.logical_not(me))
        def _():
            pltpu.make_async_copy(cv.at[s], cv.at[s], c_send.at[s]).wait()


def per_device(tile_values, tile_counts, tile_cols, panels):
    bf16, f32 = jnp.bfloat16, jnp.float32
    dma = pltpu.SemaphoreType.DMA
    depth = panels.shape[0]
    return pl.pallas_call(
        kernel,
        out_shape=jax.ShapeDtypeStruct((2 * TILE, TILE), bf16),
        in_specs=[
            pl.BlockSpec(memory_space=pl.ANY),
            pl.BlockSpec(memory_space=pl.ANY),
            pl.BlockSpec(memory_space=pl.ANY),
            pl.BlockSpec(memory_space=pl.ANY),
        ],
        out_specs=pl.BlockSpec(memory_space=pltpu.VMEM),
        scratch_shapes=[
            pltpu.SMEM((1, tile_counts.shape[0]), jnp.int32),
            pltpu.SMEM((1, tile_cols.shape[0]), jnp.int32),
            pltpu.VMEM(tile_values.shape, bf16),
            pltpu.VMEM((2 * TILE, depth), bf16),
            pltpu.VMEM((2 * TILE, depth), bf16),
            pltpu.VMEM((2, 2 * TILE, depth), bf16),
            pltpu.VMEM((STEPS, 2, depth, TILE), bf16),
            pltpu.VMEM((STEPS, NZ, PIECE, TILE), f32),
            pltpu.VMEM((STEPS, NZ, PIECE, TILE), f32),
            pltpu.VMEM((STEPS, NZ, PIECE, TILE), f32),
            pltpu.VMEM((STEPS, NZ, PIECE, TILE), f32),
            pltpu.VMEM((STEPS, NZ - 1, PIECE, TILE), f32),
            pltpu.VMEM((STEPS, PIECE, TILE), bf16),
            dma((4,)), dma, dma,
            dma((STEPS, 2)), dma((STEPS, 2)), dma((2, 2)), dma((2, 2)), dma((3,)), dma((3,)),
            dma((STEPS, 2)), dma((STEPS, 2)), dma((STEPS,)), dma((STEPS,)), dma((STEPS,)), dma,
            pltpu.SemaphoreType.REGULAR((3, 2)),
        ],
        compiler_params=pltpu.CompilerParams(
            collective_id=0, has_side_effects=True, vmem_limit_bytes=55000 * 1024
        ),
    )(tile_counts.T, tile_cols.T, tile_values, panels)


def solution(mesh):
    return jax.shard_map(
        per_device,
        mesh=mesh,
        in_specs=(P("row", "col", None), P("row", "col"), P("row", "col"), P("row", "col")),
        out_specs=P("col", "row"),
        check_vma=False,
    )
```
